512 devices in a mesh: gx: 4 (over y_lo), gy: 16 (over y_hi, z), gz: 8 (over x, core).
Axes of the slice: x: 4, y: 8 (y_hi: 2, y_lo: 4; y = y_hi * 4 + y_lo), z: 8, core: 2. Of those that a mesh axis runs over, the one named last changes fastest.
Arguments:
- grads: float32 [4, 16, 8, 160, 4096], P('gx', 'gy', 'gz'), may hold values from -6 to 6
- peer_table: int32 [16], replicated, may hold values from 0 to 15, each once
- layer_offsets: int32 [2], replicated, may hold values from 0 to 96, as said below
Outputs:
- averaged: float32 [4, 16, 8, 128, 4096], P('gx', 'gy', 'gz')
The draws below stay inside these ranges and needn't reach their ends.
Inputs may be any that keep to these rules, and one draw needn't show every extreme that they name: layer_offsets[l] is a multiple of 8 between l * (80) and l * 80 + 16; the last layer's offset is the largest of these.
All inputs are finite; a program needn't handle non-finite values.
Results may differ from the reference program's by a relative error of at most 0.00002.
Values sent between devices are 32-bit elements; how exact they have to be, the bound alone decides.
No kernel may reach another device: no remote copies, remote signals or barrier semaphores. Data moves between devices by JAX's collectives and lax.ppermute only.
A program may use at most 64 MiB of HBM per device.

```python
import jax
import jax.numpy as jnp
from jax import lax

D = 4096
ROWS = 64
LAYERS = 2
SLACK = 16
BUF = 160
GB = 8
N_GX = 4
N_GY = 16
N_GZ = 8


def draw_layer_offsets(key, part):
    steps = jax.random.randint(key, (LAYERS,), 0, SLACK // 8 + 1)
    last = jnp.arange(LAYERS, dtype=jnp.int32) == LAYERS - 1
    steps = jnp.where(last, SLACK // 8, steps)
    starts = jnp.arange(LAYERS, dtype=jnp.int32) * (ROWS + SLACK)
    return (starts + 8 * steps).astype(jnp.int32)


def block_scale(rng, shape, shards, least, largest):
    level, own = 1.0, jax.random.fold_in(rng, 6)
    for axis_at, blocks in shards:
        draws = jnp.exp(jax.random.uniform(jax.random.fold_in(own, axis_at), (blocks,), jnp.float32, least / len(shards), largest / len(shards)))
        level = level * jnp.repeat(draws, shape[axis_at] // blocks).reshape([-1 if axis == axis_at else 1 for axis in range(len(shape))])
    return level


def scatter_about(key, extent, spread, most, cuts=(), kind=jnp.bfloat16):
    factor_of = block_scale(key, extent, cuts, -0.22, 0.18) if cuts else 1.0
    result = jax.random.normal(key, extent, jnp.float32) * spread * factor_of
    return jnp.minimum(jnp.maximum(result, -most), most).astype(kind)


def setup_inputs(seed: int = 0) -> dict:
    streams_of = jax.random.split(jax.random.key(seed), 4)
    return {
        "grads": scatter_about(streams_of[0], (N_GX, N_GY, N_GZ, BUF, D), 1.0, 6.0, ((0, 4), (1, 16), (2, 8)), jnp.float32),
        "peer_table": jax.random.permutation(streams_of[1], N_GY).astype(jnp.int32),
        "layer_offsets": draw_layer_offsets(jax.random.fold_in(streams_of[3], 71), 0),
    }


def reference(grads, peer_table, layer_offsets):
    pieces = [lax.dynamic_slice_in_dim(grads, layer_offsets[i].astype(jnp.int32), ROWS, 3) for i in range(LAYERS)]
    packed = jnp.concatenate(pieces, axis=3)
    logical = jnp.take(packed, peer_table, axis=1)
    shape = logical.shape
    mean_c = jnp.mean(logical, axis=2, keepdims=True)
    mixed = 0.5 * logical + 0.5 * mean_c
    upper = shape[1] // GB
    split = mixed.reshape(shape[0], upper, GB, shape[2], shape[3], shape[4])
    mean_b = jnp.mean(split, axis=2, keepdims=True)
    split = 0.5 * split + 0.5 * mean_b
    mean_a = jnp.mean(split, axis=(0, 1), keepdims=True)
    split = 0.5 * split + 0.5 * mean_a
    mixed = split.reshape(shape)
    averaged = jnp.zeros(shape, jnp.float32).at[:, peer_table].set(mixed)
    return averaged
```

```python
import jax
import jax.numpy as jnp
from jax import lax
from jax.experimental import pallas as pl
from jax.experimental.pallas import tpu as pltpu
from jax.sharding import PartitionSpec as P

ROWS = 64
LAYERS = 2
GB = 8
SUB = 8
LANE = 128
AXES = ("gx", "gy", "gz")
VMEM = pl.BlockSpec(memory_space=pltpu.VMEM)
SMEM = pl.BlockSpec(memory_space=pltpu.SMEM)
ANY = pl.BlockSpec(memory_space=pl.ANY)
HBM = pl.BlockSpec(memory_space=pltpu.HBM)
SMALL = pltpu.CompilerParams(vmem_limit_bytes=8 * 1024 * 1024)


def pack_kernel(offsets, grads, out, sem):
    columns, lines, lane = out.shape
    copies = []
    for layer in range(LAYERS):
        start = pl.multiple_of(offsets[layer], SUB)
        for c in range(columns):
            copies.append(
                pltpu.make_async_copy(
                    grads.at[0, 0, 0, pl.ds(start, ROWS), pl.ds(c * lane, lane)],
                    out.at[c, pl.ds(layer * ROWS, ROWS), :],
                    sem,
                )
            )
    for copy in copies:
        copy.start()
    pltpu.make_async_copy(out, out, sem).wait()


def mix_kernel(table, spread, out, mixed_c, sum_b):
    n_i, n_p, n_k = spread.shape[:3]
    upper = n_p // GB
    group_a = n_i * upper

    def round_c(n, _):
        i, p = n // n_p, n % n_p
        block = spread[i, p]
        mixed_c[i, p] = 0.5 * block + (0.5 / n_k) * jnp.sum(block, axis=0, keepdims=True)
        return _

    lax.fori_loop(0, n_i * n_p, round_c, 0, unroll=4)

    def round_b(n, _):
        i, h = n // upper, n % upper
        total = mixed_c[i, table[h * GB]]
        for g in range(1, GB):
            total = total + mixed_c[i, table[h * GB + g]]
        sum_b[i, h] = total * (0.5 / GB)
        return _

    lax.fori_loop(0, n_i * upper, round_b, 0)

    def round_a(g, _):
        total = None
        for i in range(n_i):
            for h in range(upper):
                mixed_b = 0.5 * mixed_c[i, table[h * GB + g]] + sum_b[i, h]
                total = mixed_b if total is None else total + mixed_b
        total = total * (0.5 / group_a)
        for i in range(n_i):
            for h in range(upper):
                p = table[h * GB + g]
                mixed_b = 0.5 * mixed_c[i, p] + sum_b[i, h]
                out[i, p] = 0.5 * mixed_b + total
        return _

    lax.fori_loop(0, GB, round_a, 0)


def unpack_kernel(tiles, out, sem):
    columns, lines, lane = tiles.shape
    copies = [
        pltpu.make_async_copy(tiles.at[c], out.at[0, 0, 0, :, pl.ds(c * lane, lane)], sem)
        for c in range(columns)
    ]
    for copy in copies:
        copy.start()
    pltpu.make_async_copy(tiles, tiles, sem).wait()


def on_device(grads, peer_table, layer_offsets):
    n_i, n_p, n_k = (lax.axis_size(a) for a in AXES)
    peers = n_i * n_p * n_k
    width = grads.shape[-1]
    columns = width // LANE
    lines = ROWS * LAYERS
    tiles = pl.pallas_call(
        pack_kernel,
        out_shape=jax.ShapeDtypeStruct((columns, lines, LANE), jnp.float32),
        in_specs=[SMEM, HBM],
        out_specs=ANY,
        scratch_shapes=[pltpu.SemaphoreType.DMA],
        compiler_params=SMALL,
        name="pack",
    )(layer_offsets, grads)
    spread = lax.all_to_all(
        tiles.reshape(peers, -1, LANE), AXES, split_axis=0, concat_axis=0, tiled=True
    )
    per = spread.shape[1]
    block = (n_i, n_p, n_k, per, LANE)
    mixed = pl.pallas_call(
        mix_kernel,
        out_shape=jax.ShapeDtypeStruct(block, jnp.float32),
        in_specs=[SMEM, VMEM],
        out_specs=VMEM,
        scratch_shapes=[
            pltpu.VMEM(block, jnp.float32),
            pltpu.VMEM((n_i, n_p // GB, n_k, per, LANE), jnp.float32),
        ],
        compiler_params=SMALL,
        name="mix",
    )(peer_table, spread.reshape(block))
    back = lax.all_to_all(
        mixed.reshape(peers, per, LANE), AXES, split_axis=0, concat_axis=0, tiled=True
    )
    return pl.pallas_call(
        unpack_kernel,
        out_shape=jax.ShapeDtypeStruct((1, 1, 1, lines, width), jnp.float32),
        in_specs=[ANY],
        out_specs=ANY,
        scratch_shapes=[pltpu.SemaphoreType.DMA],
        compiler_params=SMALL,
        name="unpack",
    )(back.reshape(columns, lines, LANE))


def solution(mesh):
    placed = (P("gx", "gy", "gz", None, None), P(), P())
    return jax.shard_map(
        on_device,
        mesh=mesh,
        in_specs=placed,
        out_specs=P("gx", "gy", "gz", None, None),
        check_vma=False,
    )
```

```python
import jax
import jax.numpy as jnp
from jax import lax
from jax.experimental import pallas as pl
from jax.experimental.pallas import tpu as pltpu
from jax.sharding import PartitionSpec as P

ROWS = 64
LAYERS = 2
GB = 8
SUB = 8
LANE = 128
AXES = ("gx", "gy", "gz")
VMEM = pl.BlockSpec(memory_space=pltpu.VMEM)
SMEM = pl.BlockSpec(memory_space=pltpu.SMEM)
ANY = pl.BlockSpec(memory_space=pl.ANY)
SMALL = pltpu.CompilerParams(vmem_limit_bytes=8 * 1024 * 1024)


def pack_kernel(offsets, grads, out, sem):
    for layer in range(LAYERS):
        start = pl.multiple_of(offsets[layer], SUB)
        pltpu.make_async_copy(
            grads.at[0, 0, 0, pl.ds(start, ROWS), :],
            out.at[pl.ds(layer * ROWS, ROWS), :],
            sem,
        ).start()
    pltpu.make_async_copy(out, out, sem).wait()


def mix_kernel(table, spread, out, quarter, sum_b):
    n_i, n_p, n_k = spread.shape[:3]
    upper = n_p // GB
    group_a = n_i * upper

    def rounds_c_b(n, _):
        i, h = n // upper, n % upper
        total = None
        for g in range(GB):
            block = spread[i, table[h * GB + g]]
            mixed = 0.125 * block + (0.125 / n_k) * jnp.sum(block, axis=0, keepdims=True)
            quarter[i, h * GB + g] = mixed
            total = mixed if total is None else total + mixed
        sum_b[i, h] = total * (1.0 / GB)
        return _

    lax.fori_loop(0, n_i * upper, rounds_c_b, 0)

    def round_a(g, _):
        for k in range(n_k):
            mixed = [
                quarter[i, h * GB + g, k] + sum_b[i, h, k] for i in range(n_i) for h in range(upper)
            ]
            total = mixed[0]
            for value in mixed[1:]:
                total = total + value
            total = total * (1.0 / group_a)
            for i in range(n_i):
                for h in range(upper):
                    out[i, table[h * GB + g], k] = mixed[i * upper + h] + total
        return _

    lax.fori_loop(0, GB, round_a, 0)


def on_device(grads, peer_table, layer_offsets):
    n_i, n_p, n_k = (lax.axis_size(a) for a in AXES)
    peers = n_i * n_p * n_k
    width = grads.shape[-1]
    columns = width // LANE
    lines = ROWS * LAYERS
    packed = pl.pallas_call(
        pack_kernel,
        out_shape=pltpu.VMEM((lines, width), jnp.float32),
        in_specs=[SMEM, ANY],
        out_specs=ANY,
        scratch_shapes=[pltpu.SemaphoreType.DMA],
        name="pack",
    )(layer_offsets, grads)
    tiles = packed.reshape(-1, SUB, columns, LANE).transpose(0, 2, 1, 3)
    spread = lax.all_to_all(
        tiles.reshape(peers, -1, LANE), AXES, split_axis=0, concat_axis=0, tiled=True
    )
    per = spread.shape[1]
    block = (n_i, n_p, n_k, per, LANE)
    mixed = pl.pallas_call(
        mix_kernel,
        out_shape=jax.ShapeDtypeStruct(block, jnp.float32),
        in_specs=[SMEM, VMEM],
        out_specs=VMEM,
        scratch_shapes=[
            pltpu.VMEM(block, jnp.float32),
            pltpu.VMEM((n_i, n_p // GB, n_k, per, LANE), jnp.float32),
        ],
        compiler_params=SMALL,
        name="mix",
    )(peer_table, spread.reshape(block))
    back = lax.all_to_all(
        mixed.reshape(peers, per, LANE), AXES, split_axis=0, concat_axis=0, tiled=True
    )
    tiles = back.reshape(-1, columns, SUB, LANE).transpose(0, 2, 1, 3)
    return tiles.reshape(1, 1, 1, lines, width)


def solution(mesh):
    placed = (P("gx", "gy", "gz", None, None), P(), P())
    return jax.shard_map(
        on_device,
        mesh=mesh,
        in_specs=placed,
        out_specs=P("gx", "gy", "gz", None, None),
        check_vma=False,
    )
```

```python
import jax
import jax.numpy as jnp
from jax import lax
from jax.experimental import pallas as pl
from jax.experimental.pallas import tpu as pltpu
from jax.sharding import Mesh
from jax.sharding import PartitionSpec as P

ROWS = 64
LAYERS = 2
GB = 8
SUB = 8
LANE = 128
NEAR = 8
AXES = ("gx", "gy_near", "gy_far", "gz")
VMEM = pl.BlockSpec(memory_space=pltpu.VMEM)
SMEM = pl.BlockSpec(memory_space=pltpu.SMEM)
ANY = pl.BlockSpec(memory_space=pl.ANY)
SMALL = pltpu.CompilerParams(vmem_limit_bytes=8 * 1024 * 1024)


def pack_kernel(offsets, grads, out, sem):
    for layer in range(LAYERS):
        start = pl.multiple_of(offsets[layer], SUB)
        pltpu.make_async_copy(
            grads.at[0, 0, 0, pl.ds(start, ROWS), :],
            out.at[pl.ds(layer * ROWS, ROWS), :],
            sem,
        ).start()
    pltpu.make_async_copy(out, out, sem).wait()


def mix_kernel(table, spread, out, part_c, part_b):
    n_i, n_p, n_k = spread.shape[:3]
    upper = n_p // GB
    far = n_p // NEAR

    def slot(j):
        p = table[j]
        return lax.rem(p, NEAR) * far + lax.div(p, NEAR)

    def rounds_c_b(n, _):
        i, h = n // upper, n % upper
        blocks, means = None, None
        for g in range(GB):
            block = spread[i, slot(h * GB + g)]
            mean = (0.125 / n_k) * jnp.sum(block, axis=0)
            part_c[i, h * GB + g] = mean
            blocks = block if g == 0 else blocks + block
            means = mean if g == 0 else means + mean
        part_b[i, h] = (0.125 / GB) * blocks + (1.0 / GB) * means
        return _

    lax.fori_loop(0, n_i * upper, rounds_c_b, 0)

    def round_a(g, _):
        peers = [(i, h) for i in range(n_i) for h in range(upper)]
        slots = [slot(h * GB + g) for h in range(upper)]
        means = [part_c[i, h * GB + g] for i, h in peers]
        for k in range(n_k):
            mixed = [
                0.125 * spread[i, slots[h], k] + (mean + part_b[i, h, k])
                for (i, h), mean in zip(peers, means)
            ]
            terms = mixed
            while len(terms) > 1:
                terms = [sum(terms[n : n + 2][1:], terms[n]) for n in range(0, len(terms), 2)]
            total = terms[0] * (1.0 / len(peers))
            for (i, h), value in zip(peers, mixed):
                out[i, slots[h], k] = value + total
        return _

    lax.fori_loop(0, GB, round_a, 0)


def on_device(grads, peer_table, layer_offsets):
    n_i, near, far, n_k = (lax.axis_size(a) for a in AXES)
    n_p = near * far
    peers = n_i * n_p * n_k
    width = grads.shape[-1]
    columns = width // LANE
    lines = ROWS * LAYERS
    packed = pl.pallas_call(
        pack_kernel,
        out_shape=pltpu.VMEM((lines, width), jnp.float32),
        in_specs=[SMEM, ANY],
        out_specs=ANY,
        scratch_shapes=[pltpu.SemaphoreType.DMA],
        name="pack",
    )(layer_offsets, grads)
    tiles = packed.reshape(-1, SUB, columns, LANE).transpose(0, 2, 1, 3)
    spread = lax.all_to_all(
        tiles.reshape(peers, -1, LANE), AXES, split_axis=0, concat_axis=0, tiled=True
    )
    per = spread.shape[1]
    block = (n_i, n_p, n_k, per, LANE)
    mixed = pl.pallas_call(
        mix_kernel,
        out_shape=jax.ShapeDtypeStruct(block, jnp.float32),
        in_specs=[SMEM, VMEM],
        out_specs=VMEM,
        scratch_shapes=[
            pltpu.VMEM((n_i, n_p, per, LANE), jnp.float32),
            pltpu.VMEM((n_i, n_p // GB, n_k, per, LANE), jnp.float32),
        ],
        compiler_params=SMALL,
        name="mix",
    )(peer_table, spread.reshape(block))
    back = lax.all_to_all(
        mixed.reshape(peers, per, LANE), AXES, split_axis=0, concat_axis=0, tiled=True
    )
    tiles = back.reshape(-1, columns, SUB, LANE).transpose(0, 2, 1, 3)
    return tiles.reshape(1, 1, 1, lines, width)


def solution(mesh):
    gx, gy, gz = mesh.devices.shape
    fine = Mesh(mesh.devices.reshape(gx, gy // NEAR, NEAR, gz), ("gx", "gy_far", "gy_near", "gz"))
    spec = P("gx", ("gy_far", "gy_near"), "gz", None, None)
    return jax.shard_map(
        on_device, mesh=fine, in_specs=(spec, P(), P()), out_specs=spec, check_vma=False
    )
```

```python
import jax
import jax.numpy as jnp
from jax import lax
from jax.experimental import pallas as pl
from jax.experimental.pallas import tpu as pltpu
from jax.sharding import Mesh
from jax.sharding import PartitionSpec as P

ROWS = 64
LAYERS = 2
GB = 8
SUB = 8
LANE = 128
NEAR = 8
AXES = ("gx", "gy_near", "gy_far", "gz")
VMEM = pl.BlockSpec(memory_space=pltpu.VMEM)
SMEM = pl.BlockSpec(memory_space=pltpu.SMEM)
ANY = pl.BlockSpec(memory_space=pl.ANY)
SMALL = pltpu.CompilerParams(vmem_limit_bytes=8 * 1024 * 1024)


def pack_kernel(offsets, grads, out, starts, rows, sems):
    part = rows.shape[0] // LAYERS
    copies = [pltpu.make_async_copy(offsets, starts, sems.at[LAYERS])]
    for layer in range(LAYERS):
        here = pl.ds(layer * part, part)
        copies.append(
            pltpu.make_async_copy(grads.at[0, 0, 0, here, :], rows.at[here, :], sems.at[layer])
        )
    for copy in copies:
        copy.start()
    copies[0].wait()
    for layer in range(LAYERS):
        start = pl.multiple_of(starts[layer], SUB)
        copies[layer + 1].wait()
        for line in range(0, ROWS, SUB):
            out[layer * ROWS + line : layer * ROWS + line + SUB, :] = rows[
                pl.ds(pl.multiple_of(start + line, SUB), SUB), :
            ]


def mix_kernel(table, spread, out, slots, part_c, part_b):
    n_i, n_p, n_k = spread.shape[:3]
    upper = n_p // GB
    far = n_p // NEAR
    for j in range(n_p):
        p = table[j]
        slots[j] = (p & (NEAR - 1)) * far + (p >> (NEAR.bit_length() - 1))

    def rounds_c_b(i, _):
        for h in range(upper):
            blocks, means = None, None
            for g in range(GB):
                block = spread[i, slots[h * GB + g]]
                mean = (0.125 / n_k) * jnp.sum(block, axis=0)
                part_c[i, h * GB + g] = mean
                blocks = block if g == 0 else blocks + block
                means = mean if g == 0 else means + mean
            part_b[i, h] = (0.125 / GB) * blocks + (1.0 / GB) * means
        return _

    lax.fori_loop(0, n_i, rounds_c_b, 0)

    def round_a(g, _):
        peers = [(i, h) for i in range(n_i) for h in range(upper)]
        mixed = [
            0.125 * spread[i, slots[h * GB + g]]
            + (part_b[i, h] + part_c[i, h * GB + g][None])
            for i, h in peers
        ]
        terms = mixed
        while len(terms) > 1:
            terms = [terms[n] + terms[n + 1] for n in range(0, len(terms), 2)]
        total = terms[0] * (1.0 / len(peers))
        for (i, h), value in zip(peers, mixed):
            out[i, slots[h * GB + g]] = value + total
        return _

    lax.fori_loop(0, GB, round_a, 0)


def on_device(grads, peer_table, layer_offsets):
    n_i, near, far, n_k = (lax.axis_size(a) for a in AXES)
    n_p = near * far
    peers = n_i * n_p * n_k
    width = grads.shape[-1]
    columns = width // LANE
    lines = ROWS * LAYERS
    packed = pl.pallas_call(
        pack_kernel,
        out_shape=pltpu.VMEM((lines, width), jnp.float32),
        in_specs=[ANY, ANY],
        out_specs=VMEM,
        scratch_shapes=[
            pltpu.SMEM(layer_offsets.shape, jnp.int32),
            pltpu.VMEM(grads.shape[-2:], jnp.float32),
            pltpu.SemaphoreType.DMA((LAYERS + 1,)),
        ],
        name="pack",
    )(layer_offsets, grads)
    tiles = packed.reshape(-1, SUB, columns, LANE).transpose(0, 2, 1, 3)
    spread = lax.all_to_all(
        tiles.reshape(peers, -1, LANE), AXES, split_axis=0, concat_axis=0, tiled=True
    )
    per = spread.shape[1]
    block = (n_i, n_p, n_k, per, LANE)
    mixed = pl.pallas_call(
        mix_kernel,
        out_shape=jax.ShapeDtypeStruct(block, jnp.float32),
        in_specs=[SMEM, VMEM],
        out_specs=VMEM,
        scratch_shapes=[
            pltpu.SMEM((n_p,), jnp.int32),
            pltpu.VMEM((n_i, n_p, per, LANE), jnp.float32),
            pltpu.VMEM((n_i, n_p // GB, n_k, per, LANE), jnp.float32),
        ],
        compiler_params=SMALL,
        name="mix",
    )(peer_table, spread.reshape(block))
    back = lax.all_to_all(
        mixed.reshape(peers, per, LANE), AXES, split_axis=0, concat_axis=0, tiled=True
    )
    tiles = back.reshape(-1, columns, SUB, LANE).transpose(0, 2, 1, 3)
    return tiles.reshape(1, 1, 1, lines, width)


def solution(mesh):
    gx, gy, gz = mesh.devices.shape
    fine = Mesh(mesh.devices.reshape(gx, gy // NEAR, NEAR, gz), ("gx", "gy_far", "gy_near", "gz"))
    spec = P("gx", ("gy_far", "gy_near"), "gz", None, None)
    return jax.shard_map(
        on_device, mesh=fine, in_specs=(spec, P(), P()), out_specs=spec, check_vma=False
    )
```

```python
import jax
import jax.numpy as jnp
from jax import lax
from jax.experimental import pallas as pl
from jax.experimental.pallas import tpu as pltpu
from jax.sharding import Mesh
from jax.sharding import PartitionSpec as P

ROWS = 64
LAYERS = 2
GB = 8
SUB = 8
LANE = 128
NEAR = 8
CORES = 2
AXES = ("gx", "gy_near", "gy_far", "gz_core", "gz_chip")
VMEM = pl.BlockSpec(memory_space=pltpu.VMEM)
SMEM = pl.BlockSpec(memory_space=pltpu.SMEM)
ANY = pl.BlockSpec(memory_space=pl.ANY)
SMALL = pltpu.CompilerParams(vmem_limit_bytes=8 * 1024 * 1024)


def pack_kernel(offsets, grads, out, starts, rows, sems):
    part = rows.shape[0] // LAYERS
    copies = [pltpu.make_async_copy(offsets, starts, sems.at[LAYERS])]
    for layer in range(LAYERS):
        here = pl.ds(layer * part, part)
        copies.append(
            pltpu.make_async_copy(grads.at[0, 0, 0, here, :], rows.at[here, :], sems.at[layer])
        )
    for copy in copies:
        copy.start()
    copies[0].wait()
    for layer in range(LAYERS):
        start = pl.multiple_of(starts[layer], SUB)
        copies[layer + 1].wait()
        for line in range(0, ROWS, SUB):
            out[layer * ROWS + line : layer * ROWS + line + SUB, :] = rows[
                pl.ds(pl.multiple_of(start + line, SUB), SUB), :
            ]


def mix_kernel(table, spread, out, slots, part_c, part_b):
    n_i, n_p, n_k = spread.shape[:3]
    upper = n_p // GB
    far = n_p // NEAR
    for j in range(n_p):
        p = table[j]
        slots[j] = (p & (NEAR - 1)) * far + (p >> (NEAR.bit_length() - 1))

    def rounds_c_b(i, _):
        for h in range(upper):
            blocks, means = None, None
            for g in range(GB):
                block = spread[i, slots[h * GB + g]]
                mean = (0.125 / n_k) * jnp.sum(block, axis=0)
                part_c[i, h * GB + g] = mean
                blocks = block if g == 0 else blocks + block
                means = mean if g == 0 else means + mean
            part_b[i, h] = (0.125 / GB) * blocks + (1.0 / GB) * means
        return _

    lax.fori_loop(0, n_i, rounds_c_b, 0)

    def round_a(g, _):
        peers = [(i, h) for i in range(n_i) for h in range(upper)]
        mixed = [
            0.125 * spread[i, slots[h * GB + g]]
            + (part_b[i, h] + part_c[i, h * GB + g][None])
            for i, h in peers
        ]
        terms = mixed
        while len(terms) > 1:
            terms = [terms[n] + terms[n + 1] for n in range(0, len(terms), 2)]
        total = terms[0] * (1.0 / len(peers))
        for (i, h), value in zip(peers, mixed):
            out[i, slots[h * GB + g]] = value + total
        return _

    lax.fori_loop(0, GB, round_a, 0)


def on_device(grads, peer_table, layer_offsets):
    n_i, near, far, cores, chips = (lax.axis_size(a) for a in AXES)
    n_p, n_k = near * far, cores * chips
    peers = n_i * n_p * n_k
    width = grads.shape[-1]
    columns = width // LANE
    lines = ROWS * LAYERS
    packed = pl.pallas_call(
        pack_kernel,
        out_shape=pltpu.VMEM((lines, width), jnp.float32),
        in_specs=[ANY, ANY],
        out_specs=VMEM,
        scratch_shapes=[
            pltpu.SMEM(layer_offsets.shape, jnp.int32),
            pltpu.VMEM(grads.shape[-2:], jnp.float32),
            pltpu.SemaphoreType.DMA((LAYERS + 1,)),
        ],
        name="pack",
    )(layer_offsets, grads)
    tiles = packed.reshape(-1, SUB, columns, LANE).transpose(0, 2, 1, 3)
    spread = lax.all_to_all(
        tiles.reshape(peers, -1, LANE), AXES, split_axis=0, concat_axis=0, tiled=True
    )
    per = spread.shape[1]
    block = (n_i, n_p, n_k, per, LANE)
    mixed = pl.pallas_call(
        mix_kernel,
        out_shape=jax.ShapeDtypeStruct(block, jnp.float32),
        in_specs=[SMEM, VMEM],
        out_specs=VMEM,
        scratch_shapes=[
            pltpu.SMEM((n_p,), jnp.int32),
            pltpu.VMEM((n_i, n_p, per, LANE), jnp.float32),
            pltpu.VMEM((n_i, n_p // GB, n_k, per, LANE), jnp.float32),
        ],
        compiler_params=SMALL,
        name="mix",
    )(peer_table, spread.reshape(block))
    back = lax.all_to_all(
        mixed.reshape(peers, per, LANE), AXES, split_axis=0, concat_axis=0, tiled=True
    )
    tiles = back.reshape(-1, columns, SUB, LANE).transpose(0, 2, 1, 3)
    return tiles.reshape(1, 1, 1, lines, width)


def solution(mesh):
    gx, gy, gz = mesh.devices.shape
    names = ("gx", "gy_far", "gy_near", "gz_chip", "gz_core")
    shape = (gx, gy // NEAR, NEAR, gz // CORES, CORES)
    spec = P("gx", names[1:3], names[3:], None, None)
    return jax.shard_map(
        on_device,
        mesh=Mesh(mesh.devices.reshape(shape), names),
        in_specs=(spec, P(), P()),
        out_specs=spec,
        check_vma=False,
    )
```

```python
import jax
import jax.numpy as jnp
from jax import lax
from jax.experimental import pallas as pl
from jax.experimental.pallas import tpu as pltpu
from jax.sharding import PartitionSpec as P

ROWS = 64
LAYERS = 2
GB = 8
SUB = 8
LANE = 128
AXES = ("gy", "gx", "gz")
VMEM = pl.BlockSpec(memory_space=pltpu.VMEM)
SMEM = pl.BlockSpec(memory_space=pltpu.SMEM)
ANY = pl.BlockSpec(memory_space=pl.ANY)
SMALL = pltpu.CompilerParams(vmem_limit_bytes=8 * 1024 * 1024)


def pack_kernel(offsets, grads, out, starts, rows, sems):
    part = rows.shape[0] // LAYERS
    copies = [pltpu.make_async_copy(offsets, starts, sems.at[LAYERS])]
    for layer in range(LAYERS):
        here = pl.ds(layer * part, part)
        copies.append(
            pltpu.make_async_copy(grads.at[0, 0, 0, here, :], rows.at[here, :], sems.at[layer])
        )
    for copy in copies:
        copy.start()
    copies[0].wait()
    for layer in range(LAYERS):
        start = pl.multiple_of(starts[layer], SUB)
        copies[layer + 1].wait()
        for line in range(0, ROWS, SUB):
            out[layer * ROWS + line : layer * ROWS + line + SUB, :] = rows[
                pl.ds(pl.multiple_of(start + line, SUB), SUB), :
            ]


def mix_kernel(table, spread, out, part_c, part_b):
    n_p, n_i, n_k = spread.shape[:3]
    upper = n_p // GB

    def rounds_c_b(i, _):
        for h in range(upper):
            blocks, means = None, None
            for g in range(GB):
                block = spread[table[h * GB + g], i]
                mean = (0.125 / n_k) * jnp.sum(block, axis=0)
                part_c[i, h * GB + g] = mean
                blocks = block if g == 0 else blocks + block
                means = mean if g == 0 else means + mean
            part_b[i, h] = (0.125 / GB) * blocks + (1.0 / GB) * means
        return _

    lax.fori_loop(0, n_i, rounds_c_b, 0)

    def round_a(g, _):
        peers = [(i, h) for i in range(n_i) for h in range(upper)]
        mixed = [
            0.125 * spread[table[h * GB + g], i]
            + (part_b[i, h] + part_c[i, h * GB + g][None])
            for i, h in peers
        ]
        terms = mixed
        while len(terms) > 1:
            terms = [terms[n] + terms[n + 1] for n in range(0, len(terms), 2)]
        total = terms[0] * (1.0 / len(peers))
        for (i, h), value in zip(peers, mixed):
            out[table[h * GB + g], i] = value + total
        return _

    lax.fori_loop(0, GB, round_a, 0)


def on_device(grads, peer_table, layer_offsets):
    n_p, n_i, n_k = (lax.axis_size(a) for a in AXES)
    peers = n_i * n_p * n_k
    width = grads.shape[-1]
    columns = width // LANE
    lines = ROWS * LAYERS
    packed = pl.pallas_call(
        pack_kernel,
        out_shape=pltpu.VMEM((lines, width), jnp.float32),
        in_specs=[ANY, ANY],
        out_specs=VMEM,
        scratch_shapes=[
            pltpu.SMEM(layer_offsets.shape, jnp.int32),
            pltpu.VMEM(grads.shape[-2:], jnp.float32),
            pltpu.SemaphoreType.DMA((LAYERS + 1,)),
        ],
        name="pack",
    )(layer_offsets, grads)
    tiles = packed.reshape(-1, SUB, columns, LANE).transpose(0, 2, 1, 3)
    spread = lax.all_to_all(
        tiles.reshape(peers, -1, LANE), AXES, split_axis=0, concat_axis=0, tiled=True
    )
    per = spread.shape[1]
    block = (n_p, n_i, n_k, per, LANE)
    mixed = pl.pallas_call(
        mix_kernel,
        out_shape=jax.ShapeDtypeStruct(block, jnp.float32),
        in_specs=[SMEM, VMEM],
        out_specs=VMEM,
        scratch_shapes=[
            pltpu.VMEM((n_i, n_p, per, LANE), jnp.float32),
            pltpu.VMEM((n_i, n_p // GB, n_k, per, LANE), jnp.float32),
        ],
        compiler_params=SMALL,
        name="mix",
    )(peer_table, spread.reshape(block))
    back = lax.all_to_all(
        mixed.reshape(peers, per, LANE), AXES, split_axis=0, concat_axis=0, tiled=True
    )
    tiles = back.reshape(-1, columns, SUB, LANE).transpose(0, 2, 1, 3)
    return tiles.reshape(1, 1, 1, lines, width)


def solution(mesh):
    placed = P("gx", "gy", "gz", None, None)
    return jax.shard_map(
        on_device, mesh=mesh, in_specs=(placed, P(), P()), out_specs=placed, check_vma=False
    )
```
